16 devices in a mesh: dp: 2 (over y, z), tp: 8 (over x, core).
Axes of the slice: x: 4, y: 2, z: 1, core: 2. Of those that a mesh axis runs over, the one named last changes fastest.
The devices are a block of a 4x4x8 slice.
Arguments:
- x: bfloat16 [4096, 4096], P(('dp', 'tp')), parts along dimension 0
- w_gate: bfloat16 [4096, 14336], P(None, 'tp')
- w_up: bfloat16 [4096, 14336], P(None, 'tp')
- w_down: bfloat16 [14336, 4096], P('tp')
Outputs:
- output: bfloat16 [4096, 4096], P(('dp', 'tp')), parts along dimension 0
There are 2 independent parts. The reference program is written for one: setup_inputs(seed, part) draws one part's arguments, and reference() takes and returns one part's arrays. A program takes and returns all parts, laid end to end along the dimension named above; an argument that names none is the same for every part.
All inputs are finite; a program needn't handle non-finite values.
Results may differ from the reference program's by a relative error of at most 0.016.
Values are sent between devices in bfloat16 or wider.
A program may use at most 768 MiB of HBM per device.

```python
import jax
import jax.numpy as jnp

ROWS = 2048
D = 4096
FF = 14336


def setup_inputs(seed: int = 0, part: int = 0) -> dict:
    kx, kg, ku, kd = jax.random.split(jax.random.key(seed), 4)
    drawn = {
        "x": jax.random.normal(jax.random.fold_in(kx, part), (ROWS, D), jnp.float32),
        "w_gate": jax.random.normal(kg, (D, FF), jnp.float32) * D**-0.5,
        "w_up": jax.random.normal(ku, (D, FF), jnp.float32) * D**-0.5,
        "w_down": jax.random.normal(kd, (FF, D), jnp.float32) * FF**-0.5,
    }
    return {k: v.astype(jnp.bfloat16) for k, v in drawn.items()}


def reference(x, w_gate, w_up, w_down):
    gate = jnp.dot(x, w_gate, preferred_element_type=jnp.float32)
    up = jnp.dot(x, w_up, preferred_element_type=jnp.float32)
    hidden = (jax.nn.silu(gate) * up).astype(jnp.bfloat16)
    return jnp.dot(hidden, w_down, preferred_element_type=jnp.float32).astype(jnp.bfloat16)
```

```python
import functools

import jax
import jax.numpy as jnp
from jax import lax
from jax.experimental import pallas as pl
from jax.experimental.pallas import tpu as pltpu
from jax.sharding import PartitionSpec as P

MESH = pl.DeviceIdType.MESH
BF16, F32 = jnp.bfloat16, jnp.float32
BLOCKS = 4
PIECES = 4
FT = 256
NT = 4

LAND = ((1, 0), (0, 1), (1, 0))


def kernel(n, x_ref, wg_ref, wu_ref, wd_ref, y_ref, xs, wg, wu, wd, h, mine, acc, give, got, arrived,
           in_sem, w_sem, wd_sem, ag_s, ag_r, dx_s, dx_r, d2_s, d2_r, rs_s, rs_r, y_sem):
    me = lax.axis_index("tp")
    chip, core = me // 2, me % 2
    chips = n // 2
    ring = (((chip + 1) % chips) * 2 + core, ((chip + chips - 1) % chips) * 2 + core)
    partner = chip * 2 + 1 - core

    rows, depth = x_ref.shape
    half = rows // 2
    piece = half // PIECES
    steps = wg_ref.shape[1] // FT
    cols = depth // NT

    def remote(src, dst, send, recv, to):
        return pltpu.make_async_remote_copy(
            src_ref=src, dst_ref=dst, send_sem=send, recv_sem=recv, device_id={"tp": to}, device_id_type=MESH
        )

    def load_x(q):
        at = pl.ds(q * piece, piece)
        return pltpu.make_async_copy(x_ref.at[at], xs.at[0, at], in_sem.at[q])

    def gather(s, d, p):
        to = LAND[s][d] * half + p * piece
        if s == 0:
            src = xs.at[0, pl.ds(d * half + p * piece, piece)]
        elif s == 1:
            src = xs.at[1, pl.ds(LAND[0][d] * half + p * piece, piece)]
        else:
            src = xs.at[0, pl.ds((1 - d) * half + p * piece, piece)]
        return remote(src, xs.at[s + 1, pl.ds(to, piece)], ag_s.at[s, d, p], ag_r.at[s, d, p], ring[d])

    def share(b, q):
        return remote(
            xs.at[b, pl.ds(q * piece, piece)], xs.at[b, pl.ds(rows + q * piece, piece)],
            dx_s.at[b, q], dx_r.at[b, q], partner,
        )

    def pass_on(s, p):
        for d in range(2):
            gather(s, d, p).wait_recv()
            if s == 0:
                gather(1, d, p).start()
            share(s + 1, LAND[s][d] * PIECES + p).start()
        if s == 0 and p == PIECES - 1:
            for q in range(PIECES):
                for d in range(2):
                    gather(2, d, q).start()

    def load_w(slot, i):
        at = pl.ds(pl.multiple_of(i * FT, FT), FT)
        return (
            pltpu.make_async_copy(wg_ref.at[:, at], wg.at[slot], w_sem.at[slot, 0]),
            pltpu.make_async_copy(wu_ref.at[:, at], wu.at[slot], w_sem.at[slot, 1]),
        )

    def tile(j):
        return pl.ds(pl.multiple_of(j * cols, cols), cols)

    def load_wd(slot, j):
        return pltpu.make_async_copy(wd_ref.at[:, tile(j)], wd.at[slot], wd_sem.at[slot])

    def hand(b, j):
        slot = j % 2
        return remote(give.at[slot], got.at[b, :, tile(j)], d2_s.at[slot], d2_r.at[b, j], partner)

    def reduce(r, d, j):
        src = xs.at[r + 1, pl.ds(rows + d * half, half), tile(j)]
        dst = arrived.at[r, pl.ds(d * half, half), tile(j)]
        return remote(src, dst, rs_s.at[r, d, j], rs_r.at[r, d, j], ring[d])

    def combine(b, j):
        hand(b, j).wait_recv()
        total = mine[j % 2] + got[b, :, tile(j)].astype(F32)
        if b == BLOCKS - 1:
            for d in range(2):
                reduce(1, d, j).wait_recv()
            total = total + arrived[1, :, tile(j)].astype(F32)
        xs[b, rows:, tile(j)] = total.astype(BF16)
        for d in range(2):
            reduce(b - 1, d, j).start()

    beside = {
        (0, 0, 2): [(0, 0)], (0, 0, 5): [(0, 1)], (0, 1, 0): [(0, 2)], (0, 1, 2): [(0, 3)],
        (1, 0, 1): [(1, 0)], (1, 0, 3): [(1, 1)], (1, 0, 5): [(1, 2)], (1, 1, 1): [(1, 3)],
        (2, 0, 0): [(2, 0)], (2, 0, 1): [(2, 1)], (2, 0, 3): [(2, 2)], (2, 0, 5): [(2, 3)],
    }

    def run_beside(b, phase, i):
        for (b_, phase_, step), pieces in beside.items():
            if (b_, phase_) == (b, phase):
                @pl.when(i == step)
                def _():
                    for s, p in pieces:
                        pass_on(s, p)

    for c in load_w(0, 0):
        c.start()
    for q in range(2 * PIECES):
        load_x(q).start()
    barrier = pltpu.get_barrier_semaphore()
    for to in (*ring, partner):
        pl.semaphore_signal(barrier, inc=1, device_id={"tp": to}, device_id_type=MESH)
    pl.semaphore_wait(barrier, 3)
    for p in range(PIECES):
        for d in range(2):
            q = d * PIECES + p
            load_x(q).wait()
            gather(0, d, p).start()
            share(0, q).start()

    for b in range(BLOCKS):
        for q in range(2 * PIECES):
            share(b, q).wait_recv()

        def project(i, _, b=b):
            at = b * steps + i
            slot = at % 2
            for c in load_w(slot, i):
                c.wait()

            @pl.when(at + 1 < BLOCKS * steps)
            def _():
                for c in load_w(1 - slot, (i + 1) % steps):
                    c.start()

            @pl.when(i == 0)
            def _():
                load_wd((b * NT) % 2, 0).start()

            if b >= 2:
                @pl.when(i == 1)
                def _():
                    combine(b - 1, NT - 1)

            run_beside(b, 0, i)
            x = xs[b]
            gate = jnp.dot(x, wg[slot], preferred_element_type=F32)
            up = jnp.dot(x, wu[slot], preferred_element_type=F32)
            h[:, pl.ds(pl.multiple_of(i * FT, FT), FT)] = (jax.nn.silu(gate) * up).astype(BF16)
            return 0

        lax.fori_loop(0, steps, project, 0)

        def contract(j, _, b=b):
            slot = (b * NT + j) % 2
            load_wd(slot, j).wait()

            @pl.when(j + 1 < NT)
            def _():
                load_wd(1 - slot, j + 1).start()

            run_beside(b, 1, j)
            if b > 0:
                @pl.when(j > 0)
                def _():
                    combine(b, j - 1)

            @pl.when(b * NT + j >= 2)
            def _():
                hand(b, j).wait_send()

            term = jnp.dot(h[...], wd[slot], preferred_element_type=F32)
            give[j % 2] = term[rows:].astype(BF16)
            if b == 0:
                acc[:, tile(j)] = term[:rows]
            else:
                mine[j % 2] = term[:rows]
            hand(b, j).start()
            return 0

        lax.fori_loop(0, NT, contract, 0)

    combine(BLOCKS - 1, NT - 1)

    def early(j, _):
        hand(0, j).wait_recv()
        for d in range(2):
            reduce(0, d, j).wait_recv()
        for d in range(2):
            at = pl.ds(d * half, half)
            other = pl.ds((1 - d) * half, half)
            acc[at, tile(j)] = (
                acc[at, tile(j)] + got[0, at, tile(j)].astype(F32) + arrived[0, other, tile(j)].astype(F32)
            )
        return 0

    lax.fori_loop(0, NT, early, 0)

    def store_y(j):
        return pltpu.make_async_copy(xs.at[0, rows:, tile(j)], y_ref.at[:, tile(j)], y_sem.at[j])

    def finish(j, _):
        for d in range(2):
            reduce(2, d, j).wait_recv()
        xs[0, rows:, tile(j)] = (acc[:, tile(j)] + arrived[2, :, tile(j)].astype(F32)).astype(BF16)
        store_y(j).start()
        return 0

    lax.fori_loop(0, NT, finish, 0)

    for j in range(NT):
        for d in range(2):
            for r in range(3):
                reduce(r, d, j).wait_send()
    for j in range(2):
        hand(BLOCKS - 1, j).wait_send()
    for s in range(3):
        for d in range(2):
            for p in range(PIECES):
                gather(s, d, p).wait_send()
    for b in range(BLOCKS):
        for q in range(2 * PIECES):
            share(b, q).wait_send()
    for j in range(NT):
        store_y(j).wait()


def solution(mesh):
    n = mesh.shape["tp"]

    def step(x, w_gate, w_up, w_down):
        rows, depth = x.shape
        units = w_gate.shape[1]
        cols = depth // NT
        dma = pltpu.SemaphoreType.DMA
        return pl.pallas_call(
            functools.partial(kernel, n),
            name="mlp",
            out_shape=jax.ShapeDtypeStruct((rows, depth), BF16),
            in_specs=[pl.BlockSpec(memory_space=pl.ANY)] * 4,
            out_specs=pl.BlockSpec(memory_space=pl.ANY),
            scratch_shapes=[
                pltpu.VMEM((BLOCKS, 2 * rows, depth), BF16),
                pltpu.VMEM((2, depth, FT), BF16),
                pltpu.VMEM((2, depth, FT), BF16),
                pltpu.VMEM((2, units, cols), BF16),
                pltpu.VMEM((2 * rows, units), BF16),
                pltpu.VMEM((2, rows, cols), F32),
                pltpu.VMEM((rows, depth), F32),
                pltpu.VMEM((2, rows, cols), BF16),
                pltpu.VMEM((BLOCKS, rows, depth), BF16),
                pltpu.VMEM((3, rows, depth), BF16),
                dma((2 * PIECES,)), dma((2, 2)), dma((2,)),
                dma((3, 2, PIECES)), dma((3, 2, PIECES)),
                dma((BLOCKS, 2 * PIECES)), dma((BLOCKS, 2 * PIECES)),
                dma((2,)), dma((BLOCKS, NT)),
                dma((3, 2, NT)), dma((3, 2, NT)), dma((NT,)),
            ],
            compiler_params=pltpu.CompilerParams(
                collective_id=0, has_side_effects=True, vmem_limit_bytes=67043328
            ),
        )(x, w_gate, w_up, w_down)

    return jax.shard_map(
        step,
        mesh=mesh,
        in_specs=(P(("dp", "tp"), None), P(None, "tp"), P(None, "tp"), P("tp", None)),
        out_specs=P(("dp", "tp"), None),
        check_vma=False,
    )
```

```python
import functools

import jax
import jax.numpy as jnp
from jax import lax
from jax.experimental import pallas as pl
from jax.experimental.pallas import tpu as pltpu
from jax.sharding import PartitionSpec as P

MESH = pl.DeviceIdType.MESH
BF16, F32 = jnp.bfloat16, jnp.float32
BLOCKS = 4
PIECES = 4
FT = 256
NT = 4

LAND = ((1, 0), (0, 1), (1, 0))


def kernel(n, x_ref, wg_ref, wu_ref, wd_ref, y_ref, xs, wg, wu, wd, h, mine, acc, give, got, arrived,
           in_sem, w_sem, wd_sem, ag_s, ag_r, dx_s, dx_r, d2_s, d2_r, rs_s, n1_r, rs_r, y_sem):
    me = lax.axis_index("tp")
    chip, core = me // 2, me % 2
    chips = n // 2
    ring = (((chip + 1) % chips) * 2 + core, ((chip + chips - 1) % chips) * 2 + core)
    partner = chip * 2 + 1 - core

    rows, depth = x_ref.shape
    half = rows // 2
    piece = half // PIECES
    steps = wg_ref.shape[1] // FT
    cols = depth // NT

    def remote(src, dst, send, recv, to):
        return pltpu.make_async_remote_copy(
            src_ref=src, dst_ref=dst, send_sem=send, recv_sem=recv, device_id={"tp": to}, device_id_type=MESH
        )

    def load_x(q):
        at = pl.ds(q * piece, piece)
        return pltpu.make_async_copy(x_ref.at[at], xs.at[0, at], in_sem.at[q])

    def gather(s, d, p):
        to = LAND[s][d] * half + p * piece
        if s == 0:
            src = xs.at[0, pl.ds(d * half + p * piece, piece)]
        elif s == 1:
            src = xs.at[1, pl.ds(LAND[0][d] * half + p * piece, piece)]
        else:
            src = xs.at[0, pl.ds((1 - d) * half + p * piece, piece)]
        return remote(src, xs.at[s + 1, pl.ds(to, piece)], ag_s, ag_r.at[s, d, p], ring[d])

    def share(b, q):
        return remote(
            xs.at[b, pl.ds(q * piece, piece)], xs.at[b, pl.ds(rows + q * piece, piece)],
            dx_s, dx_r.at[b], partner,
        )

    def landed(ref, sem):
        pltpu.make_async_copy(ref, ref, sem).wait()

    def pass_on(s, p):
        for d in range(2):
            gather(s, d, p).wait_recv()
            if s == 0:
                gather(1, d, p).start()
            share(s + 1, LAND[s][d] * PIECES + p).start()
        if s == 0 and p == PIECES - 1:
            for q in range(PIECES):
                for d in range(2):
                    gather(2, d, q).start()

    def load_w(slot, i):
        at = pl.ds(pl.multiple_of(i * FT, FT), FT)
        return (
            pltpu.make_async_copy(wg_ref.at[:, at], wg.at[slot], w_sem.at[slot, 0]),
            pltpu.make_async_copy(wu_ref.at[:, at], wu.at[slot], w_sem.at[slot, 1]),
        )

    def tile(j):
        return pl.ds(pl.multiple_of(j * cols, cols), cols)

    def load_wd(slot, j):
        return pltpu.make_async_copy(wd_ref.at[:, tile(j)], wd.at[slot], wd_sem.at[slot])

    def hand(b, j):
        slot = j % 2
        return remote(give.at[slot], got.at[b, :, tile(j)], d2_s.at[slot], d2_r.at[b, j], partner)

    def reduce(r, d, j):
        src = xs.at[r + 1, pl.ds(rows + d * half, half), tile(j)]
        dst = arrived.at[r, pl.ds(d * half, half), tile(j)]
        return remote(src, dst, rs_s, n1_r if r == 0 else rs_r.at[r - 1, d, j], ring[d])

    def combine(b, j):
        hand(b, j).wait_recv()
        total = mine[j % 2] + got[b, :, tile(j)].astype(F32)
        if b == BLOCKS - 1:
            for d in range(2):
                reduce(1, d, j).wait_recv()
            total = total + arrived[1, :, tile(j)].astype(F32)
        xs[b, rows:, tile(j)] = total.astype(BF16)
        for d in range(2):
            reduce(b - 1, d, j).start()

    beside = {
        (0, 0, 2): [(0, 0)], (0, 0, 5): [(0, 1)], (0, 1, 0): [(0, 2)], (0, 1, 2): [(0, 3)],
        (1, 0, 1): [(1, 0)], (1, 0, 3): [(1, 1)], (1, 0, 5): [(1, 2)], (1, 1, 1): [(1, 3)],
        (2, 0, 0): [(2, 0)], (2, 0, 1): [(2, 1)], (2, 0, 3): [(2, 2)], (2, 0, 5): [(2, 3)],
    }

    def run_beside(b, phase, i):
        for (b_, phase_, step), pieces in beside.items():
            if (b_, phase_) == (b, phase):
                @pl.when(i == step)
                def _():
                    for s, p in pieces:
                        pass_on(s, p)

    for c in load_w(0, 0):
        c.start()
    for q in range(2 * PIECES):
        load_x(q).start()
    barrier = pltpu.get_barrier_semaphore()
    for to in (*ring, partner):
        pl.semaphore_signal(barrier, inc=1, device_id={"tp": to}, device_id_type=MESH)
    pl.semaphore_wait(barrier, 3)
    for p in range(PIECES):
        for d in range(2):
            q = d * PIECES + p
            load_x(q).wait()
            gather(0, d, p).start()
            share(0, q).start()

    for b in range(BLOCKS):
        landed(xs.at[b, pl.ds(rows, rows)], dx_r.at[b])

        def project(i, _, b=b):
            at = b * steps + i
            slot = at % 2
            for c in load_w(slot, i):
                c.wait()

            @pl.when(at + 1 < BLOCKS * steps)
            def _():
                for c in load_w(1 - slot, (i + 1) % steps):
                    c.start()

            @pl.when(i == 0)
            def _():
                load_wd((b * NT) % 2, 0).start()

            if b >= 2:
                @pl.when(i == 1)
                def _():
                    combine(b - 1, NT - 1)

            run_beside(b, 0, i)
            x = xs[b]
            gate = jnp.dot(x, wg[slot], preferred_element_type=F32)
            up = jnp.dot(x, wu[slot], preferred_element_type=F32)
            h[:, pl.ds(pl.multiple_of(i * FT, FT), FT)] = (jax.nn.silu(gate) * up).astype(BF16)
            return 0

        lax.fori_loop(0, steps, project, 0)

        def contract(j, _, b=b):
            slot = (b * NT + j) % 2
            load_wd(slot, j).wait()

            @pl.when(j + 1 < NT)
            def _():
                load_wd(1 - slot, j + 1).start()

            run_beside(b, 1, j)

            @pl.when(b * NT + j >= 2)
            def _():
                hand(b, j).wait_send()

            term = jnp.dot(h[...], wd[slot], preferred_element_type=F32)
            give[j % 2] = term[rows:].astype(BF16)
            if b == 0:
                acc[:, tile(j)] = term[:rows]
            else:
                mine[j % 2] = term[:rows]
            hand(b, j).start()
            if b > 0:
                @pl.when(j > 0)
                def _():
                    combine(b, j - 1)

            return 0

        lax.fori_loop(0, NT, contract, 0)

    combine(BLOCKS - 1, NT - 1)

    landed(arrived.at[0], n1_r)

    def early(j, _):
        hand(0, j).wait_recv()
        for d in range(2):
            at = pl.ds(d * half, half)
            other = pl.ds((1 - d) * half, half)
            acc[at, tile(j)] = (
                acc[at, tile(j)] + got[0, at, tile(j)].astype(F32) + arrived[0, other, tile(j)].astype(F32)
            )
        return 0

    lax.fori_loop(0, NT, early, 0)

    def store_y(j):
        return pltpu.make_async_copy(xs.at[0, rows:, tile(j)], y_ref.at[:, tile(j)], y_sem)

    def finish(j, _):
        for d in range(2):
            reduce(2, d, j).wait_recv()
        xs[0, rows:, tile(j)] = (acc[:, tile(j)] + arrived[2, :, tile(j)].astype(F32)).astype(BF16)
        store_y(j).start()
        return 0

    lax.fori_loop(0, NT, finish, 0)

    landed(arrived, rs_s)
    landed(arrived, ag_s)
    for j in range(2):
        hand(BLOCKS - 1, j).wait_send()
    landed(xs.at[:, pl.ds(0, rows)], dx_s)
    landed(xs.at[0, pl.ds(rows, rows)], y_sem)


def solution(mesh):
    n = mesh.shape["tp"]

    def step(x, w_gate, w_up, w_down):
        rows, depth = x.shape
        units = w_gate.shape[1]
        cols = depth // NT
        dma = pltpu.SemaphoreType.DMA
        return pl.pallas_call(
            functools.partial(kernel, n),
            name="mlp",
            out_shape=jax.ShapeDtypeStruct((rows, depth), BF16),
            in_specs=[pl.BlockSpec(memory_space=pl.ANY)] * 4,
            out_specs=pl.BlockSpec(memory_space=pl.ANY),
            scratch_shapes=[
                pltpu.VMEM((BLOCKS, 2 * rows, depth), BF16),
                pltpu.VMEM((2, depth, FT), BF16),
                pltpu.VMEM((2, depth, FT), BF16),
                pltpu.VMEM((2, units, cols), BF16),
                pltpu.VMEM((2 * rows, units), BF16),
                pltpu.VMEM((2, rows, cols), F32),
                pltpu.VMEM((rows, depth), F32),
                pltpu.VMEM((2, rows, cols), BF16),
                pltpu.VMEM((BLOCKS, rows, depth), BF16),
                pltpu.VMEM((3, rows, depth), BF16),
                dma((2 * PIECES,)), dma((2, 2)), dma((2,)),
                dma, dma((3, 2, PIECES)),
                dma, dma((BLOCKS,)),
                dma((2,)), dma((BLOCKS, NT)),
                dma, dma, dma((2, 2, NT)), dma,
            ],
            compiler_params=pltpu.CompilerParams(
                collective_id=0, has_side_effects=True, vmem_limit_bytes=67043328
            ),
        )(x, w_gate, w_up, w_down)

    return jax.shard_map(
        step,
        mesh=mesh,
        in_specs=(P(("dp", "tp"), None), P(None, "tp"), P(None, "tp"), P("tp", None)),
        out_specs=P(("dp", "tp"), None),
        check_vma=False,
    )
```

```python
import functools

import jax
import jax.numpy as jnp
from jax import lax
from jax.experimental import pallas as pl
from jax.experimental.pallas import tpu as pltpu
from jax.sharding import PartitionSpec as P

MESH = pl.DeviceIdType.MESH
BF16, F32 = jnp.bfloat16, jnp.float32
BLOCKS = 4
PIECES = 4
FT = 256
NT = 4

LAND = ((1, 0), (0, 1), (1, 0))


def kernel(n, x_ref, wg_ref, wu_ref, wd_ref, y_ref, xs, wg, wu, wd, h, mine, acc, give, got, arrived,
           in_sem, w_sem, wd_sem, ag_s, ag_r, dx_s, dx_r, d2_s, d2_r, rs_s, n1_r, rs_r):
    me = lax.axis_index("tp")
    chip, core = me // 2, me % 2
    chips = n // 2
    ring = (((chip + 1) % chips) * 2 + core, ((chip + chips - 1) % chips) * 2 + core)
    partner = chip * 2 + 1 - core

    rows, depth = x_ref.shape
    half = rows // 2
    piece = half // PIECES
    steps = wg_ref.shape[1] // FT
    cols = depth // NT

    def remote(src, dst, send, recv, to):
        return pltpu.make_async_remote_copy(
            src_ref=src, dst_ref=dst, send_sem=send, recv_sem=recv, device_id={"tp": to}, device_id_type=MESH
        )

    def load_x(q):
        at = pl.ds(q * piece, piece)
        return pltpu.make_async_copy(x_ref.at[at], xs.at[0, at], in_sem.at[q])

    def gather(s, d, p):
        to = LAND[s][d] * half + p * piece
        if s == 0:
            src = xs.at[0, pl.ds(d * half + p * piece, piece)]
        elif s == 1:
            src = xs.at[1, pl.ds(LAND[0][d] * half + p * piece, piece)]
        else:
            src = xs.at[0, pl.ds((1 - d) * half + p * piece, piece)]
        return remote(src, xs.at[s + 1, pl.ds(to, piece)], ag_s, ag_r.at[s, d, p], ring[d])

    def share(b, q):
        return remote(
            xs.at[b, pl.ds(q * piece, piece)], xs.at[b, pl.ds(rows + q * piece, piece)],
            dx_s, dx_r.at[b], partner,
        )

    def landed(ref, sem):
        pltpu.make_async_copy(ref, ref, sem).wait()

    def pass_on(s, p):
        for d in range(2):
            gather(s, d, p).wait_recv()
            if s == 0:
                gather(1, d, p).start()
            share(s + 1, LAND[s][d] * PIECES + p).start()
        if s == 0 and p == PIECES - 1:
            for q in range(PIECES):
                for d in range(2):
                    gather(2, d, q).start()

    def load_w(slot, i):
        at = pl.ds(pl.multiple_of(i * FT, FT), FT)
        return (
            pltpu.make_async_copy(wg_ref.at[:, at], wg.at[slot], w_sem.at[slot, 0]),
            pltpu.make_async_copy(wu_ref.at[:, at], wu.at[slot], w_sem.at[slot, 1]),
        )

    def tile(j):
        return pl.ds(pl.multiple_of(j * cols, cols), cols)

    def load_wd(slot, j):
        return pltpu.make_async_copy(wd_ref.at[:, tile(j)], wd.at[slot], wd_sem.at[slot])

    def hand(b, j):
        slot = j % 2
        return remote(give.at[slot], got.at[b, :, tile(j)], d2_s.at[slot], d2_r.at[b, j], partner)

    def reduce(r, d, j):
        src = xs.at[r + 1, pl.ds(rows + d * half, half), tile(j)]
        dst = arrived.at[r, pl.ds(d * half, half), tile(j)]
        return remote(src, dst, rs_s, n1_r if r == 0 else rs_r.at[r - 1, d, j], ring[d])

    def combine(b, j):
        hand(b, j).wait_recv()
        total = mine[j % 2] + got[b, :, tile(j)].astype(F32)
        if b == BLOCKS - 1:
            for d in range(2):
                reduce(1, d, j).wait_recv()
            total = total + arrived[1, :, tile(j)].astype(F32)
        xs[b, rows:, tile(j)] = total.astype(BF16)
        for d in range(2):
            reduce(b - 1, d, j).start()

    beside = {
        (0, 0, 2): [(0, 0)], (0, 0, 5): [(0, 1)], (0, 1, 0): [(0, 2)], (0, 1, 2): [(0, 3)],
        (1, 0, 1): [(1, 0)], (1, 0, 3): [(1, 1)], (1, 0, 5): [(1, 2)], (1, 1, 1): [(1, 3)],
        (2, 0, 0): [(2, 0)], (2, 0, 1): [(2, 1)], (2, 0, 3): [(2, 2)], (2, 0, 5): [(2, 3)],
    }

    def run_beside(b, phase, i):
        for (b_, phase_, step), pieces in beside.items():
            if (b_, phase_) == (b, phase):
                @pl.when(i == step)
                def _():
                    for s, p in pieces:
                        pass_on(s, p)

    for c in load_w(0, 0):
        c.start()
    for q in range(2 * PIECES):
        load_x(q).start()
    barrier = pltpu.get_barrier_semaphore()
    for to in (*ring, partner):
        pl.semaphore_signal(barrier, inc=1, device_id={"tp": to}, device_id_type=MESH)
    pl.semaphore_wait(barrier, 3)
    for p in range(PIECES):
        for d in range(2):
            q = d * PIECES + p
            load_x(q).wait()
            gather(0, d, p).start()
            share(0, q).start()

    for b in range(BLOCKS):
        landed(xs.at[b, pl.ds(rows, rows)], dx_r.at[b])

        def project(i, _, b=b):
            at = b * steps + i
            slot = at % 2
            for c in load_w(slot, i):
                c.wait()

            @pl.when(at + 1 < BLOCKS * steps)
            def _():
                for c in load_w(1 - slot, (i + 1) % steps):
                    c.start()

            @pl.when(i == 0)
            def _():
                load_wd((b * NT) % 2, 0).start()

            if b >= 2:
                @pl.when(i == 1)
                def _():
                    combine(b - 1, NT - 1)

            run_beside(b, 0, i)
            x = xs[b]
            gate = jnp.dot(x, wg[slot], preferred_element_type=F32)
            up = jnp.dot(x, wu[slot], preferred_element_type=F32)
            h[:, pl.ds(pl.multiple_of(i * FT, FT), FT)] = (jax.nn.silu(gate) * up).astype(BF16)
            return 0

        lax.fori_loop(0, steps, project, 0)

        def contract(j, _, b=b):
            slot = (b * NT + j) % 2
            load_wd(slot, j).wait()

            @pl.when(j + 1 < NT)
            def _():
                load_wd(1 - slot, j + 1).start()

            run_beside(b, 1, j)

            @pl.when(b * NT + j >= 2)
            def _():
                hand(b, j).wait_send()

            term = jnp.dot(h[...], wd[slot], preferred_element_type=F32)
            give[j % 2] = term[rows:].astype(BF16)
            if b == 0:
                acc[:, tile(j)] = term[:rows]
            else:
                mine[j % 2] = term[:rows]
            hand(b, j).start()
            if b > 0:
                @pl.when(j > 0)
                def _():
                    combine(b, j - 1)

            return 0

        lax.fori_loop(0, NT, contract, 0)

    combine(BLOCKS - 1, NT - 1)

    landed(arrived.at[0], n1_r)

    def early(j, _):
        hand(0, j).wait_recv()
        for d in range(2):
            at = pl.ds(d * half, half)
            other = pl.ds((1 - d) * half, half)
            acc[at, tile(j)] = (
                acc[at, tile(j)] + got[0, at, tile(j)].astype(F32) + arrived[0, other, tile(j)].astype(F32)
            )
        return 0

    lax.fori_loop(0, NT, early, 0)

    def finish(j, _):
        for d in range(2):
            reduce(2, d, j).wait_recv()
        y_ref[:, tile(j)] = (acc[:, tile(j)] + arrived[2, :, tile(j)].astype(F32)).astype(BF16)
        return 0

    lax.fori_loop(0, NT, finish, 0)

    landed(arrived, rs_s)
    landed(arrived, ag_s)
    for j in range(2):
        hand(BLOCKS - 1, j).wait_send()
    landed(xs.at[:, pl.ds(0, rows)], dx_s)


def solution(mesh):
    n = mesh.shape["tp"]

    def step(x, w_gate, w_up, w_down):
        rows, depth = x.shape
        units = w_gate.shape[1]
        cols = depth // NT
        dma = pltpu.SemaphoreType.DMA
        return pl.pallas_call(
            functools.partial(kernel, n),
            name="mlp",
            out_shape=pltpu.VMEM((rows, depth), BF16),
            in_specs=[pl.BlockSpec(memory_space=pl.ANY)] * 4,
            out_specs=pl.BlockSpec(memory_space=pltpu.VMEM),
            scratch_shapes=[
                pltpu.VMEM((BLOCKS, 2 * rows, depth), BF16),
                pltpu.VMEM((2, depth, FT), BF16),
                pltpu.VMEM((2, depth, FT), BF16),
                pltpu.VMEM((2, units, cols), BF16),
                pltpu.VMEM((2 * rows, units), BF16),
                pltpu.VMEM((2, rows, cols), F32),
                pltpu.VMEM((rows, depth), F32),
                pltpu.VMEM((2, rows, cols), BF16),
                pltpu.VMEM((BLOCKS, rows, depth), BF16),
                pltpu.VMEM((3, rows, depth), BF16),
                dma((2 * PIECES,)), dma((2, 2)), dma((2,)),
                dma, dma((3, 2, PIECES)),
                dma, dma((BLOCKS,)),
                dma((2,)), dma((BLOCKS, NT)),
                dma, dma, dma((2, 2, NT)),
            ],
            compiler_params=pltpu.CompilerParams(
                collective_id=0, has_side_effects=True, vmem_limit_bytes=62914560
            ),
        )(x, w_gate, w_up, w_down)

    return jax.shard_map(
        step,
        mesh=mesh,
        in_specs=(P(("dp", "tp"), None), P(None, "tp"), P(None, "tp"), P("tp", None)),
        out_specs=P(("dp", "tp"), None),
        check_vma=False,
    )
```

```python
import functools

import jax
import jax.numpy as jnp
from jax import lax
from jax.experimental import pallas as pl
from jax.experimental.pallas import tpu as pltpu
from jax.sharding import PartitionSpec as P

MESH = pl.DeviceIdType.MESH
BF16, F32 = jnp.bfloat16, jnp.float32
BLOCKS = 4
PIECES = 4
FT = 256
NT = 4

LAND = ((1, 0), (0, 1), (1, 0))


def kernel(n, x_ref, wg_ref, wu_ref, wd_ref, y_ref, xs, wg, wu, wd, h, mine, acc, give, got, arrived,
           in_sem, w_sem, wd_sem, ag_s, ag_r, dx_s, dx_r, d2_s, d0_r, d2_r, rs_s, n1_r, rs_r):
    me = lax.axis_index("tp")
    chip, core = me // 2, me % 2
    chips = n // 2
    ring = (((chip + 1) % chips) * 2 + core, ((chip + chips - 1) % chips) * 2 + core)
    partner = chip * 2 + 1 - core

    rows, depth = x_ref.shape
    half = rows // 2
    piece = half // PIECES
    steps = wg_ref.shape[1] // FT
    cols = depth // NT

    def remote(src, dst, send, recv, to):
        return pltpu.make_async_remote_copy(
            src_ref=src, dst_ref=dst, send_sem=send, recv_sem=recv, device_id={"tp": to}, device_id_type=MESH
        )

    def load_x(q):
        at = pl.ds(q * piece, piece)
        return pltpu.make_async_copy(x_ref.at[at], xs.at[0, at], in_sem.at[q])

    def gather(s, d, p):
        to = LAND[s][d] * half + p * piece
        if s == 0:
            src = xs.at[0, pl.ds(d * half + p * piece, piece)]
        elif s == 1:
            src = xs.at[1, pl.ds(LAND[0][d] * half + p * piece, piece)]
        else:
            src = xs.at[0, pl.ds((1 - d) * half + p * piece, piece)]
        return remote(src, xs.at[s + 1, pl.ds(to, piece)], ag_s, ag_r.at[p if s == 0 else PIECES + s - 1], ring[d])

    def share(b, q):
        return remote(
            xs.at[b, pl.ds(q * piece, piece)], xs.at[b, pl.ds(rows + q * piece, piece)],
            dx_s, dx_r.at[b], partner,
        )

    def landed(ref, sem):
        pltpu.make_async_copy(ref, ref, sem).wait()

    def pass_on(s, p):
        if s == 0:
            landed(xs.at[1, pl.ds(0, 2 * piece)], ag_r.at[p])
            for d in range(2):
                gather(1, d, p).start()
                share(1, LAND[0][d] * PIECES + p).start()
            if p == PIECES - 1:
                for q in range(PIECES):
                    for d in range(2):
                        gather(2, d, q).start()
        else:
            landed(xs.at[s + 1, pl.ds(0, rows)], ag_r.at[PIECES + s - 1])
            for q in range(2 * PIECES):
                share(s + 1, q).start()

    def load_w(slot, i):
        at = pl.ds(pl.multiple_of(i * FT, FT), FT)
        return (
            pltpu.make_async_copy(wg_ref.at[:, at], wg.at[slot], w_sem.at[slot, 0]),
            pltpu.make_async_copy(wu_ref.at[:, at], wu.at[slot], w_sem.at[slot, 1]),
        )

    def tile(j):
        return pl.ds(pl.multiple_of(j * cols, cols), cols)

    def load_wd(slot, j):
        return pltpu.make_async_copy(wd_ref.at[:, tile(j)], wd.at[slot], wd_sem.at[slot])

    def hand(b, j):
        slot = j % 2
        return remote(give.at[slot], got.at[b, :, tile(j)], d2_s.at[slot], d0_r if b == 0 else d2_r.at[b - 1, j], partner)

    def reduce(r, d, j):
        src = xs.at[r + 1, pl.ds(rows + d * half, half), tile(j)]
        dst = arrived.at[r, pl.ds(d * half, half), tile(j)]
        return remote(src, dst, rs_s, n1_r if r == 0 else rs_r.at[r - 1, j], ring[d])

    def combine(b, j):
        hand(b, j).wait_recv()
        total = mine[j % 2] + got[b, :, tile(j)].astype(F32)
        if b == BLOCKS - 1:
            landed(arrived.at[1, :, tile(j)], rs_r.at[0, j])
            total = total + arrived[1, :, tile(j)].astype(F32)
        xs[b, rows:, tile(j)] = total.astype(BF16)
        for d in range(2):
            reduce(b - 1, d, j).start()

    beside = {
        (0, 0, 2): [(0, 0)], (0, 0, 5): [(0, 1)], (0, 1, 0): [(0, 2)], (0, 1, 2): [(0, 3)],
        (1, 1, 1): [(1, 0)], (2, 0, 6): [(2, 0)],
    }

    def run_beside(b, phase, i):
        for (b_, phase_, step), pieces in beside.items():
            if (b_, phase_) == (b, phase):
                @pl.when(i == step)
                def _():
                    for s, p in pieces:
                        pass_on(s, p)

    barrier = pltpu.get_barrier_semaphore()
    for to in (*ring, partner):
        pl.semaphore_signal(barrier, inc=1, device_id={"tp": to}, device_id_type=MESH)
    for p in range(PIECES):
        for d in range(2):
            load_x(d * PIECES + p).start()
    pl.semaphore_wait(barrier, 3)
    for p in range(PIECES):
        for d in range(2):
            q = d * PIECES + p
            load_x(q).wait()
            gather(0, d, p).start()
            share(0, q).start()
    for c in load_w(0, 0):
        c.start()

    for b in range(BLOCKS):
        landed(xs.at[b, pl.ds(rows, rows)], dx_r.at[b])

        def project(i, _, b=b):
            at = b * steps + i
            slot = at % 2
            for c in load_w(slot, i):
                c.wait()

            @pl.when(at + 1 < BLOCKS * steps)
            def _():
                for c in load_w(1 - slot, (i + 1) % steps):
                    c.start()

            @pl.when(i == 0)
            def _():
                load_wd((b * NT) % 2, 0).start()

            if b >= 2:
                @pl.when(i == 1)
                def _():
                    combine(b - 1, NT - 1)

            run_beside(b, 0, i)
            x = xs[b]
            gate = jnp.dot(x, wg[slot], preferred_element_type=F32)
            up = jnp.dot(x, wu[slot], preferred_element_type=F32)
            h[:, pl.ds(pl.multiple_of(i * FT, FT), FT)] = (jax.nn.silu(gate) * up).astype(BF16)
            return 0

        lax.fori_loop(0, steps, project, 0)

        def contract(j, _, b=b):
            slot = (b * NT + j) % 2
            load_wd(slot, j).wait()

            @pl.when(j + 1 < NT)
            def _():
                load_wd(1 - slot, j + 1).start()

            run_beside(b, 1, j)

            @pl.when(b * NT + j >= 2)
            def _():
                hand(b, j).wait_send()

            term = jnp.dot(h[...], wd[slot], preferred_element_type=F32)
            give[j % 2] = term[rows:].astype(BF16)
            if b == 0:
                acc[:, tile(j)] = term[:rows]
            else:
                mine[j % 2] = term[:rows]
            hand(b, j).start()
            if b > 0:
                @pl.when(j > 0)
                def _():
                    combine(b, j - 1)

            return 0

        lax.fori_loop(0, NT, contract, 0)

    combine(BLOCKS - 1, NT - 1)

    landed(got.at[0], d0_r)
    landed(arrived.at[0], n1_r)

    def early(j, _):
        for d in range(2):
            at = pl.ds(d * half, half)
            other = pl.ds((1 - d) * half, half)
            acc[at, tile(j)] = (
                acc[at, tile(j)] + got[0, at, tile(j)].astype(F32) + arrived[0, other, tile(j)].astype(F32)
            )
        return 0

    lax.fori_loop(0, NT, early, 0)

    def finish(j, _):
        landed(arrived.at[2, :, tile(j)], rs_r.at[1, j])
        y_ref[:, tile(j)] = (acc[:, tile(j)] + arrived[2, :, tile(j)].astype(F32)).astype(BF16)
        return 0

    lax.fori_loop(0, NT, finish, 0)

    landed(arrived, rs_s)
    landed(arrived, ag_s)
    for j in range(2):
        hand(BLOCKS - 1, j).wait_send()
    landed(xs.at[:, pl.ds(0, rows)], dx_s)


def solution(mesh):
    n = mesh.shape["tp"]

    def step(x, w_gate, w_up, w_down):
        rows, depth = x.shape
        units = w_gate.shape[1]
        cols = depth // NT
        dma = pltpu.SemaphoreType.DMA
        return pl.pallas_call(
            functools.partial(kernel, n),
            name="mlp",
            out_shape=pltpu.VMEM((rows, depth), BF16),
            in_specs=[pl.BlockSpec(memory_space=pl.ANY)] * 4,
            out_specs=pl.BlockSpec(memory_space=pltpu.VMEM),
            scratch_shapes=[
                pltpu.VMEM((BLOCKS, 2 * rows, depth), BF16),
                pltpu.VMEM((2, depth, FT), BF16),
                pltpu.VMEM((2, depth, FT), BF16),
                pltpu.VMEM((2, units, cols), BF16),
                pltpu.VMEM((2 * rows, units), BF16),
                pltpu.VMEM((2, rows, cols), F32),
                pltpu.VMEM((rows, depth), F32),
                pltpu.VMEM((2, rows, cols), BF16),
                pltpu.VMEM((BLOCKS, rows, depth), BF16),
                pltpu.VMEM((3, rows, depth), BF16),
                dma((2 * PIECES,)), dma((2, 2)), dma((2,)),
                dma, dma((PIECES + 2,)),
                dma, dma((BLOCKS,)),
                dma((2,)), dma, dma((BLOCKS - 1, NT)),
                dma, dma, dma((2, NT)),
            ],
            compiler_params=pltpu.CompilerParams(
                collective_id=0, has_side_effects=True, vmem_limit_bytes=62914560
            ),
        )(x, w_gate, w_up, w_down)

    return jax.shard_map(
        step,
        mesh=mesh,
        in_specs=(P(("dp", "tp"), None), P(None, "tp"), P(None, "tp"), P("tp", None)),
        out_specs=P(("dp", "tp"), None),
        check_vma=False,
    )
```

```python
import functools

import jax
import jax.numpy as jnp
from jax import lax
from jax.experimental import pallas as pl
from jax.experimental.pallas import tpu as pltpu
from jax.sharding import PartitionSpec as P

MESH = pl.DeviceIdType.MESH
BF16, F32 = jnp.bfloat16, jnp.float32
BLOCKS = 4
PIECES = 4
FT = 256
NT = 4
LAST = 256

LAND = ((1, 0), (0, 1), (1, 0))


def kernel(n, x_ref, wg_ref, wu_ref, wd_ref, y_ref, xs, wgu, wd, h, mine, acc, give, got, arrived,
           in_sem, w_sem, wd_sem, ag_s, ag_r, dx_s, dx_r, d2_s, own_r, d2_r, rs_s, rs_r):
    me = lax.axis_index("tp")
    chip, core = me // 2, me % 2
    chips = n // 2
    ring = (((chip + 1) % chips) * 2 + core, ((chip + chips - 1) % chips) * 2 + core)
    partner = chip * 2 + 1 - core

    rows, depth = x_ref.shape
    half = rows // 2
    piece = half // PIECES
    steps = wg_ref.shape[1] // FT
    cols = depth // NT
    first, last = pl.ds(depth - cols, cols - LAST), pl.ds(depth - LAST, LAST)

    def remote(src, dst, send, recv, to):
        return pltpu.make_async_remote_copy(
            src_ref=src, dst_ref=dst, send_sem=send, recv_sem=recv, device_id={"tp": to}, device_id_type=MESH
        )

    def load_x(q):
        at = pl.ds(q * piece, piece)
        return pltpu.make_async_copy(x_ref.at[at], xs.at[0, at], in_sem.at[0 if q % PIECES == 0 else 1])

    def gather(s, d, p):
        to = LAND[s][d] * half + p * piece
        if s == 0:
            src = xs.at[0, pl.ds(d * half + p * piece, piece)]
        elif s == 1:
            src = xs.at[1, pl.ds(LAND[0][d] * half + p * piece, piece)]
        else:
            src = xs.at[0, pl.ds((1 - d) * half + p * piece, piece)]
        return remote(src, xs.at[s + 1, pl.ds(to, piece)], ag_s, ag_r.at[p if s == 0 else PIECES + s - 1], ring[d])

    def share(b, q):
        return remote(
            xs.at[b, pl.ds(q * piece, piece)], xs.at[b, pl.ds(rows + q * piece, piece)],
            dx_s, dx_r.at[b % 2], partner,
        )

    def landed(ref, sem):
        pltpu.make_async_copy(ref, ref, sem).wait()

    def pass_on(s, p):
        if s == 0:
            landed(xs.at[1, pl.ds(0, 2 * piece)], ag_r.at[p])
            for d in range(2):
                gather(1, d, p).start()
                share(1, LAND[0][d] * PIECES + p).start()
            if p == PIECES - 1:
                for q in range(PIECES):
                    for d in range(2):
                        gather(2, d, q).start()
        else:
            landed(xs.at[s + 1, pl.ds(0, rows)], ag_r.at[PIECES + s - 1])
            for q in range(2 * PIECES):
                share(s + 1, q).start()

    def load_w(slot, i):
        at = pl.ds(pl.multiple_of(i * FT, FT), FT)
        return (
            pltpu.make_async_copy(wg_ref.at[:, at], wgu.at[slot, 0], w_sem.at[slot]),
            pltpu.make_async_copy(wu_ref.at[:, at], wgu.at[slot, 1], w_sem.at[slot]),
        )

    def tile(j):
        return pl.ds(pl.multiple_of(j * cols, cols), cols)

    def load_wd(slot, j):
        return pltpu.make_async_copy(wd_ref.at[:, tile(j)], wd.at[slot], wd_sem.at[slot])

    def hand(b, j):
        slot = j % 2
        return remote(give.at[slot], got.at[b, :, tile(j)], d2_s.at[slot], own_r if b == 0 else d2_r.at[b % 2, j], partner)

    def reduce(r, d, columns, sem):
        src = xs.at[r + 1, pl.ds(rows + d * half, half), columns]
        dst = arrived.at[r, pl.ds(d * half, half), columns]
        return remote(src, dst, rs_s, sem, ring[d])

    def send_on(r, j):
        if r < 2:
            for d in range(2):
                reduce(r, d, tile(j), own_r if r == 0 else rs_r.at[0, j // 2]).start()
            return

        @pl.when(j < NT - 1)
        def _():
            for d in range(2):
                reduce(2, d, tile(j), rs_r.at[1, 0]).start()

        @pl.when(j == NT - 1)
        def _():
            for columns, at in ((first, 0), (last, 1)):
                for d in range(2):
                    reduce(2, d, columns, rs_r.at[1, at]).start()

    def combine(b, j):
        hand(b, j).wait_recv()
        total = mine[j % 2] + got[b, :, tile(j)].astype(F32)
        if b == BLOCKS - 1:
            @pl.when(j % 2 == 0)
            def _():
                landed(arrived.at[1, :, pl.ds(0, 2 * cols)], rs_r.at[0, j // 2])

            total = total + arrived[1, :, tile(j)].astype(F32)
        xs[b, rows:, tile(j)] = total.astype(BF16)
        send_on(b - 1, j)

    beside = {
        (0, 0, 2): [(0, 0)], (0, 0, 5): [(0, 1)], (0, 1, 0): [(0, 2)], (0, 1, 2): [(0, 3)],
        (1, 1, 1): [(1, 0)], (2, 0, 6): [(2, 0)],
    }

    def run_beside(b, phase, i):
        for (b_, phase_, step), pieces in beside.items():
            if (b_, phase_) == (b, phase):
                @pl.when(i == step)
                def _():
                    for s, p in pieces:
                        pass_on(s, p)

    barrier = pltpu.get_barrier_semaphore()
    for to in (*ring, partner):
        pl.semaphore_signal(barrier, inc=1, device_id={"tp": to}, device_id_type=MESH)
    for p in range(PIECES):
        for d in range(2):
            load_x(d * PIECES + p).start()
    pl.semaphore_wait(barrier, 3)
    for p in range(PIECES):
        if p < 2:
            landed(xs.at[0, pl.ds(0, 2 * (piece if p == 0 else half - piece))], in_sem.at[p])
        for d in range(2):
            gather(0, d, p).start()
            share(0, d * PIECES + p).start()
    for c in load_w(0, 0):
        c.start()

    for b in range(BLOCKS):
        landed(xs.at[b, pl.ds(rows, rows)], dx_r.at[b % 2])

        def project(i, _, b=b):
            at = b * steps + i
            slot = at % 2
            landed(wgu.at[slot], w_sem.at[slot])

            @pl.when(at + 1 < BLOCKS * steps)
            def _():
                for c in load_w(1 - slot, (i + 1) % steps):
                    c.start()

            @pl.when(i == 0)
            def _():
                load_wd((b * NT) % 2, 0).start()

            if b >= 2:
                @pl.when(i == 1)
                def _():
                    combine(b - 1, NT - 1)

            run_beside(b, 0, i)
            x = xs[b]
            gate = jnp.dot(x, wgu[slot, 0], preferred_element_type=F32)
            up = jnp.dot(x, wgu[slot, 1], preferred_element_type=F32)
            h[:, pl.ds(pl.multiple_of(i * FT, FT), FT)] = (jax.nn.silu(gate) * up).astype(BF16)
            return 0

        lax.fori_loop(0, steps, project, 0)

        def contract(j, _, b=b):
            slot = (b * NT + j) % 2
            load_wd(slot, j).wait()

            @pl.when(j + 1 < NT)
            def _():
                load_wd(1 - slot, j + 1).start()

            run_beside(b, 1, j)

            @pl.when(b * NT + j >= 2)
            def _():
                hand(b, j).wait_send()

            term = jnp.dot(h[...], wd[slot], preferred_element_type=F32)
            give[j % 2] = term[rows:].astype(BF16)
            if b == 0:
                acc[:, tile(j)] = term[:rows]
            else:
                mine[j % 2] = term[:rows]
            hand(b, j).start()
            if b > 0:
                @pl.when(j > 0)
                def _():
                    combine(b, j - 1)

            return 0

        lax.fori_loop(0, NT, contract, 0)

    combine(BLOCKS - 1, NT - 1)

    landed(arrived, ag_s)
    landed(xs.at[:, pl.ds(0, rows)], dx_s)
    landed(xs.at[0], own_r)

    def early(j, _):
        for d in range(2):
            at = pl.ds(d * half, half)
            other = pl.ds((1 - d) * half, half)
            acc[at, tile(j)] = (
                acc[at, tile(j)] + got[0, at, tile(j)].astype(F32) + arrived[0, other, tile(j)].astype(F32)
            )
        return 0

    lax.fori_loop(0, NT, early, 0)

    def finish(columns):
        y_ref[:, columns] = (acc[:, columns] + arrived[2, :, columns].astype(F32)).astype(BF16)

    rest = pl.ds(0, depth - LAST)
    landed(arrived.at[2, :, rest], rs_r.at[1, 0])
    finish(rest)
    landed(arrived.at[2, :, last], rs_r.at[1, 1])
    finish(last)

    landed(arrived, rs_s)
    for j in range(2):
        hand(BLOCKS - 1, j).wait_send()


def solution(mesh):
    n = mesh.shape["tp"]

    def step(x, w_gate, w_up, w_down):
        rows, depth = x.shape
        units = w_gate.shape[1]
        cols = depth // NT
        dma = pltpu.SemaphoreType.DMA
        return pl.pallas_call(
            functools.partial(kernel, n),
            name="mlp",
            out_shape=pltpu.VMEM((rows, depth), BF16),
            in_specs=[pl.BlockSpec(memory_space=pl.ANY)] * 4,
            out_specs=pl.BlockSpec(memory_space=pltpu.VMEM),
            scratch_shapes=[
                pltpu.VMEM((BLOCKS, 2 * rows, depth), BF16),
                pltpu.VMEM((2, 2, depth, FT), BF16),
                pltpu.VMEM((2, units, cols), BF16),
                pltpu.VMEM((2 * rows, units), BF16),
                pltpu.VMEM((2, rows, cols), F32),
                pltpu.VMEM((rows, depth), F32),
                pltpu.VMEM((2, rows, cols), BF16),
                pltpu.VMEM((BLOCKS, rows, depth), BF16),
                pltpu.VMEM((3, rows, depth), BF16),
                dma((2,)), dma((2,)), dma((2,)),
                dma, dma((PIECES + 2,)),
                dma, dma((2,)),
                dma((2,)), dma, dma((2, NT)),
                dma, dma((2, 2)),
            ],
            compiler_params=pltpu.CompilerParams(
                collective_id=0, has_side_effects=True, vmem_limit_bytes=62914560
            ),
        )(x, w_gate, w_up, w_down)

    return jax.shard_map(
        step,
        mesh=mesh,
        in_specs=(P(("dp", "tp"), None), P(None, "tp"), P(None, "tp"), P("tp", None)),
        out_specs=P(("dp", "tp"), None),
        check_vma=False,
    )
```

```python
import functools

import jax
import jax.numpy as jnp
from jax import lax
from jax.experimental import pallas as pl
from jax.experimental.pallas import tpu as pltpu
from jax.sharding import PartitionSpec as P

MESH = pl.DeviceIdType.MESH
BF16, F32 = jnp.bfloat16, jnp.float32
BLOCKS = 4
PIECES = 4
FT = 256
NT = 4
LAST = 256

LAND = ((1, 0), (0, 1), (1, 0))


def kernel(n, x_ref, wg_ref, wu_ref, wd_ref, y_ref, xs, wgu, wd, h, mine, acc, give, got, arrived,
           in_sem, w_sem, wd_sem, ag_s, ag_r, dx_s, dx_r, d2_s, own_r, d2_r, rs_s, rs_r):
    me = lax.axis_index("tp")
    chip, core = me // 2, me % 2
    chips = n // 2
    ring = (((chip + 1) % chips) * 2 + core, ((chip + chips - 1) % chips) * 2 + core)
    partner = chip * 2 + 1 - core

    rows, depth = x_ref.shape
    half = rows // 2
    piece = half // PIECES
    steps = wg_ref.shape[1] // FT
    cols = depth // NT
    first, last = pl.ds(depth - cols, cols - LAST), pl.ds(depth - LAST, LAST)

    def remote(src, dst, send, recv, to):
        return pltpu.make_async_remote_copy(
            src_ref=src, dst_ref=dst, send_sem=send, recv_sem=recv, device_id={"tp": to}, device_id_type=MESH
        )

    def load_x(q):
        at = pl.ds(q * piece, piece)
        return pltpu.make_async_copy(x_ref.at[at], xs.at[0, at], in_sem.at[0 if q % PIECES == 0 else 1])

    def gather(s, d, p):
        to = LAND[s][d] * half + p * piece
        if s == 0:
            src = x_ref.at[pl.ds(d * half + p * piece, piece)]
        elif s == 1:
            src = xs.at[1, pl.ds(LAND[0][d] * half + p * piece, piece)]
        else:
            src = xs.at[0, pl.ds((1 - d) * half + p * piece, piece)]
        return remote(src, xs.at[s + 1, pl.ds(to, piece)], ag_s, ag_r.at[p if s == 0 else PIECES + s - 1], ring[d])

    def share(b, q):
        return remote(
            xs.at[b, pl.ds(q * piece, piece)], xs.at[b, pl.ds(rows + q * piece, piece)],
            dx_s, dx_r.at[b % 2], partner,
        )

    def landed(ref, sem):
        pltpu.make_async_copy(ref, ref, sem).wait()

    def pass_on(s, p):
        if s == 0:
            landed(xs.at[1, pl.ds(0, 2 * piece)], ag_r.at[p])
            for d in range(2):
                gather(1, d, p).start()
                share(1, LAND[0][d] * PIECES + p).start()
            if p == PIECES - 1:
                for q in range(PIECES):
                    for d in range(2):
                        gather(2, d, q).start()
        else:
            landed(xs.at[s + 1, pl.ds(0, rows)], ag_r.at[PIECES + s - 1])
            for q in range(2 * PIECES):
                share(s + 1, q).start()

    def load_w(slot, i):
        at = pl.ds(pl.multiple_of(i * FT, FT), FT)
        return (
            pltpu.make_async_copy(wg_ref.at[:, at], wgu.at[slot, 0], w_sem.at[slot]),
            pltpu.make_async_copy(wu_ref.at[:, at], wgu.at[slot, 1], w_sem.at[slot]),
        )

    def tile(j):
        return pl.ds(pl.multiple_of(j * cols, cols), cols)

    def load_wd(slot, j):
        return pltpu.make_async_copy(wd_ref.at[:, tile(j)], wd.at[slot], wd_sem.at[slot])

    def hand(b, j):
        slot = j % 2
        return remote(give.at[slot], got.at[b, :, tile(j)], d2_s.at[slot], own_r if b == 0 else d2_r.at[b % 2, j], partner)

    def reduce(r, d, columns, sem):
        src = xs.at[r + 1, pl.ds(rows + d * half, half), columns]
        dst = arrived.at[r, pl.ds(d * half, half), columns]
        return remote(src, dst, rs_s, sem, ring[d])

    def send_on(r, j):
        if r < 2:
            for d in range(2):
                reduce(r, d, tile(j), own_r if r == 0 else rs_r.at[0, j // 2]).start()
            return

        @pl.when(j < NT - 1)
        def _():
            for d in range(2):
                reduce(2, d, tile(j), rs_r.at[1, 0]).start()

        @pl.when(j == NT - 1)
        def _():
            for columns, at in ((first, 0), (last, 1)):
                for d in range(2):
                    reduce(2, d, columns, rs_r.at[1, at]).start()

    def combine(b, j):
        hand(b, j).wait_recv()
        total = mine[j % 2] + got[b, :, tile(j)].astype(F32)
        if b == BLOCKS - 1:
            @pl.when(j % 2 == 0)
            def _():
                landed(arrived.at[1, :, pl.ds(0, 2 * cols)], rs_r.at[0, j // 2])

            total = total + arrived[1, :, tile(j)].astype(F32)
        xs[b, rows:, tile(j)] = total.astype(BF16)
        send_on(b - 1, j)

    beside = {
        (0, 0, 2): [(0, 0)], (0, 0, 5): [(0, 1)], (0, 1, 0): [(0, 2)], (0, 1, 2): [(0, 3)],
        (1, 1, 1): [(1, 0)], (2, 0, 6): [(2, 0)],
    }

    def run_beside(b, phase, i):
        for (b_, phase_, step), pieces in beside.items():
            if (b_, phase_) == (b, phase):
                @pl.when(i == step)
                def _():
                    for s, p in pieces:
                        pass_on(s, p)

    barrier = pltpu.get_barrier_semaphore()
    for to in (*ring, partner):
        pl.semaphore_signal(barrier, inc=1, device_id={"tp": to}, device_id_type=MESH)
    for p in range(PIECES):
        for d in range(2):
            load_x(d * PIECES + p).start()
    pl.semaphore_wait(barrier, 3)
    for p in range(PIECES):
        for d in range(2):
            gather(0, d, p).start()
    for p in range(2):
        landed(xs.at[0, pl.ds(0, 2 * (piece if p == 0 else half - piece))], in_sem.at[p])
    for q in range(2 * PIECES):
        share(0, q).start()
    for c in load_w(0, 0):
        c.start()

    for b in range(BLOCKS):
        landed(xs.at[b, pl.ds(rows, rows)], dx_r.at[b % 2])

        def project(i, _, b=b):
            at = b * steps + i
            slot = at % 2
            landed(wgu.at[slot], w_sem.at[slot])

            @pl.when(at + 1 < BLOCKS * steps)
            def _():
                for c in load_w(1 - slot, (i + 1) % steps):
                    c.start()

            @pl.when(i == 0)
            def _():
                load_wd((b * NT) % 2, 0).start()

            if b >= 2:
                @pl.when(i == 1)
                def _():
                    combine(b - 1, NT - 1)

            run_beside(b, 0, i)
            x = xs[b]
            gate = jnp.dot(x, wgu[slot, 0], preferred_element_type=F32)
            up = jnp.dot(x, wgu[slot, 1], preferred_element_type=F32)
            h[:, pl.ds(pl.multiple_of(i * FT, FT), FT)] = (jax.nn.silu(gate) * up).astype(BF16)
            return 0

        lax.fori_loop(0, steps, project, 0)

        def contract(j, _, b=b):
            slot = (b * NT + j) % 2
            load_wd(slot, j).wait()

            @pl.when(j + 1 < NT)
            def _():
                load_wd(1 - slot, j + 1).start()

            run_beside(b, 1, j)

            @pl.when(b * NT + j >= 2)
            def _():
                hand(b, j).wait_send()

            term = jnp.dot(h[...], wd[slot], preferred_element_type=F32)
            give[j % 2] = term[rows:].astype(BF16)
            if b == 0:
                acc[:, tile(j)] = term[:rows]
            else:
                mine[j % 2] = term[:rows]
            hand(b, j).start()
            if b > 0:
                @pl.when(j > 0)
                def _():
                    combine(b, j - 1)

            return 0

        lax.fori_loop(0, NT, contract, 0)

    combine(BLOCKS - 1, NT - 1)

    landed(arrived, ag_s)
    landed(xs.at[:, pl.ds(0, rows)], dx_s)
    landed(xs.at[0], own_r)

    def early(j, _):
        for d in range(2):
            at = pl.ds(d * half, half)
            other = pl.ds((1 - d) * half, half)
            acc[at, tile(j)] = (
                acc[at, tile(j)] + got[0, at, tile(j)].astype(F32) + arrived[0, other, tile(j)].astype(F32)
            )
        return 0

    lax.fori_loop(0, NT, early, 0)

    def finish(columns):
        y_ref[:, columns] = (acc[:, columns] + arrived[2, :, columns].astype(F32)).astype(BF16)

    rest = pl.ds(0, depth - LAST)
    landed(arrived.at[2, :, rest], rs_r.at[1, 0])
    finish(rest)
    landed(arrived.at[2, :, last], rs_r.at[1, 1])
    finish(last)

    landed(arrived, rs_s)
    for j in range(2):
        hand(BLOCKS - 1, j).wait_send()


def solution(mesh):
    n = mesh.shape["tp"]

    def step(x, w_gate, w_up, w_down):
        rows, depth = x.shape
        units = w_gate.shape[1]
        cols = depth // NT
        dma = pltpu.SemaphoreType.DMA
        return pl.pallas_call(
            functools.partial(kernel, n),
            name="mlp",
            out_shape=pltpu.VMEM((rows, depth), BF16),
            in_specs=[pl.BlockSpec(memory_space=pl.ANY)] * 4,
            out_specs=pl.BlockSpec(memory_space=pltpu.VMEM),
            scratch_shapes=[
                pltpu.VMEM((BLOCKS, 2 * rows, depth), BF16),
                pltpu.VMEM((2, 2, depth, FT), BF16),
                pltpu.VMEM((2, units, cols), BF16),
                pltpu.VMEM((2 * rows, units), BF16),
                pltpu.VMEM((2, rows, cols), F32),
                pltpu.VMEM((rows, depth), F32),
                pltpu.VMEM((2, rows, cols), BF16),
                pltpu.VMEM((BLOCKS, rows, depth), BF16),
                pltpu.VMEM((3, rows, depth), BF16),
                dma((2,)), dma((2,)), dma((2,)),
                dma, dma((PIECES + 2,)),
                dma, dma((2,)),
                dma((2,)), dma, dma((2, NT)),
                dma, dma((2, 2)),
            ],
            compiler_params=pltpu.CompilerParams(
                collective_id=0, has_side_effects=True, vmem_limit_bytes=62914560
            ),
        )(x, w_gate, w_up, w_down)

    return jax.shard_map(
        step,
        mesh=mesh,
        in_specs=(P(("dp", "tp"), None), P(None, "tp"), P(None, "tp"), P("tp", None)),
        out_specs=P(("dp", "tp"), None),
        check_vma=False,
    )
```

```python
import functools

import jax
import jax.numpy as jnp
from jax import lax
from jax.experimental import pallas as pl
from jax.experimental.pallas import tpu as pltpu
from jax.sharding import PartitionSpec as P

MESH = pl.DeviceIdType.MESH
BF16, F32 = jnp.bfloat16, jnp.float32
BLOCKS = 4
PIECES = 2
FT = 256
NT = 4
LAST = 128

LAND = ((1, 0), (0, 1), (1, 0))


def kernel(n, x_ref, wg_ref, wu_ref, wd_ref, y_ref, xs, wgu, wd, h, mine, acc, give, got, arrived,
           in_sem, w_sem, wd_sem, ag_s, ag_r, dx_s, dx_r, d2_s, own_r, d2_r, rs_s, rs_r):
    me = lax.axis_index("tp")
    chip, core = me // 2, me % 2
    chips = n // 2
    ring = (((chip + 1) % chips) * 2 + core, ((chip + chips - 1) % chips) * 2 + core)
    partner = chip * 2 + 1 - core

    rows, depth = x_ref.shape
    half = rows // 2
    piece = half // PIECES
    steps = wg_ref.shape[1] // FT
    cols = depth // NT
    first, last = pl.ds(depth - cols, cols - LAST), pl.ds(depth - LAST, LAST)

    def remote(src, dst, send, recv, to):
        return pltpu.make_async_remote_copy(
            src_ref=src, dst_ref=dst, send_sem=send, recv_sem=recv, device_id={"tp": to}, device_id_type=MESH
        )

    def load_x(q):
        at = pl.ds(q * piece, piece)
        return pltpu.make_async_copy(x_ref.at[at], xs.at[0, at], in_sem.at[0 if q % PIECES == 0 else 1])

    def gather(s, d, p):
        to = LAND[s][d] * half + p * piece
        if s == 0:
            src = x_ref.at[pl.ds(d * half + p * piece, piece)]
        elif s == 1:
            src = xs.at[1, pl.ds(LAND[0][d] * half + p * piece, piece)]
        else:
            src = xs.at[0, pl.ds((1 - d) * half + p * piece, piece)]
        return remote(src, xs.at[s + 1, pl.ds(to, piece)], ag_s, ag_r.at[p if s == 0 else PIECES + s - 1], ring[d])

    def share(b, q):
        return remote(
            xs.at[b, pl.ds(q * piece, piece)], xs.at[b, pl.ds(rows + q * piece, piece)],
            dx_s, dx_r.at[b % 2], partner,
        )

    def landed(ref, sem):
        pltpu.make_async_copy(ref, ref, sem).wait()

    def pass_on(s, p):
        if s == 0:
            landed(xs.at[1, pl.ds(0, 2 * piece)], ag_r.at[p])
            for d in range(2):
                gather(1, d, p).start()
                share(1, LAND[0][d] * PIECES + p).start()
            if p == PIECES - 1:
                for q in range(PIECES):
                    for d in range(2):
                        gather(2, d, q).start()
        else:
            landed(xs.at[s + 1, pl.ds(0, rows)], ag_r.at[PIECES + s - 1])
            for q in range(2 * PIECES):
                share(s + 1, q).start()

    def load_w(slot, i):
        at = pl.ds(pl.multiple_of(i * FT, FT), FT)
        return (
            pltpu.make_async_copy(wg_ref.at[:, at], wgu.at[slot, 0], w_sem.at[slot]),
            pltpu.make_async_copy(wu_ref.at[:, at], wgu.at[slot, 1], w_sem.at[slot]),
        )

    def tile(j):
        return pl.ds(pl.multiple_of(j * cols, cols), cols)

    def load_wd(slot, j):
        return pltpu.make_async_copy(wd_ref.at[:, tile(j)], wd.at[slot], wd_sem.at[slot])

    def hand(b, j):
        slot = j % 2
        return remote(give.at[slot], got.at[b, :, tile(j)], d2_s.at[slot], own_r if b == 0 else d2_r.at[b % 2, j], partner)

    def reduce(r, d, columns, sem):
        src = xs.at[r + 1, pl.ds(rows + d * half, half), columns]
        dst = arrived.at[r, pl.ds(d * half, half), columns]
        return remote(src, dst, rs_s, sem, ring[d])

    def send_on(r, j):
        if r < 2:
            for d in range(2):
                reduce(r, d, tile(j), own_r if r == 0 else rs_r.at[0, j // 2]).start()
            return

        @pl.when(j < NT - 1)
        def _():
            for d in range(2):
                reduce(2, d, tile(j), rs_r.at[1, 0]).start()

        @pl.when(j == NT - 1)
        def _():
            for columns, at in ((first, 0), (last, 1)):
                for d in range(2):
                    reduce(2, d, columns, rs_r.at[1, at]).start()

    def combine(b, j):
        hand(b, j).wait_recv()
        total = mine[j % 2] + got[b, :, tile(j)].astype(F32)
        if b == BLOCKS - 1:
            @pl.when(j % 2 == 0)
            def _():
                landed(arrived.at[1, :, pl.ds(0, 2 * cols)], rs_r.at[0, j // 2])

            total = total + arrived[1, :, tile(j)].astype(F32)
        xs[b, rows:, tile(j)] = total.astype(BF16)
        send_on(b - 1, j)

    beside = {
        (0, 0, 6): [(0, 0)], (0, 1, 2): [(0, 1)],
        (1, 1, 1): [(1, 0)], (2, 0, 6): [(2, 0)],
    }

    def run_beside(b, phase, i):
        for (b_, phase_, step), pieces in beside.items():
            if (b_, phase_) == (b, phase):
                @pl.when(i == step)
                def _():
                    for s, p in pieces:
                        pass_on(s, p)

    barrier = pltpu.get_barrier_semaphore()
    for to in (*ring, partner):
        pl.semaphore_signal(barrier, inc=1, device_id={"tp": to}, device_id_type=MESH)
    for p in range(PIECES):
        for d in range(2):
            load_x(d * PIECES + p).start()
    pl.semaphore_wait(barrier, 3)
    for p in range(PIECES):
        for d in range(2):
            gather(0, d, p).start()
    for p in range(2):
        landed(xs.at[0, pl.ds(0, 2 * (piece if p == 0 else half - piece))], in_sem.at[p])
    for q in range(2 * PIECES):
        share(0, q).start()
    for c in load_w(0, 0):
        c.start()

    for b in range(BLOCKS):
        landed(xs.at[b, pl.ds(rows, rows)], dx_r.at[b % 2])

        def project(i, _, b=b):
            at = b * steps + i
            slot = at % 2
            landed(wgu.at[slot], w_sem.at[slot])

            @pl.when(at + 1 < BLOCKS * steps)
            def _():
                for c in load_w(1 - slot, (i + 1) % steps):
                    c.start()

            @pl.when(i == 0)
            def _():
                load_wd((b * NT) % 2, 0).start()

            if b >= 2:
                @pl.when(i == 1)
                def _():
                    combine(b - 1, NT - 1)

            run_beside(b, 0, i)
            x = xs[b]
            gate = jnp.dot(x, wgu[slot, 0], preferred_element_type=F32)
            up = jnp.dot(x, wgu[slot, 1], preferred_element_type=F32)
            h[:, pl.ds(pl.multiple_of(i * FT, FT), FT)] = (jax.nn.silu(gate) * up).astype(BF16)
            return 0

        lax.fori_loop(0, steps, project, 0)

        def contract(j, _, b=b):
            slot = (b * NT + j) % 2
            load_wd(slot, j).wait()

            @pl.when(j + 1 < NT)
            def _():
                load_wd(1 - slot, j + 1).start()

            run_beside(b, 1, j)

            @pl.when(b * NT + j >= 2)
            def _():
                hand(b, j).wait_send()

            term = jnp.dot(h[...], wd[slot], preferred_element_type=F32)
            give[j % 2] = term[rows:].astype(BF16)
            if b == 0:
                acc[:, tile(j)] = term[:rows]
            else:
                mine[j % 2] = term[:rows]
            hand(b, j).start()
            if b > 0:
                @pl.when(j > 0)
                def _():
                    combine(b, j - 1)

            return 0

        lax.fori_loop(0, NT, contract, 0)

    combine(BLOCKS - 1, NT - 1)

    landed(arrived, ag_s)
    landed(xs.at[:, pl.ds(0, rows)], dx_s)
    landed(xs.at[0], own_r)

    def early(j, _):
        for d in range(2):
            at = pl.ds(d * half, half)
            other = pl.ds((1 - d) * half, half)
            acc[at, tile(j)] = (
                acc[at, tile(j)] + got[0, at, tile(j)].astype(F32) + arrived[0, other, tile(j)].astype(F32)
            )
        return 0

    lax.fori_loop(0, NT, early, 0)

    def finish(columns):
        y_ref[:, columns] = (acc[:, columns] + arrived[2, :, columns].astype(F32)).astype(BF16)

    rest = pl.ds(0, depth - LAST)
    landed(arrived.at[2, :, rest], rs_r.at[1, 0])
    finish(rest)
    landed(arrived.at[2, :, last], rs_r.at[1, 1])
    finish(last)

    landed(arrived, rs_s)
    for j in range(2):
        hand(BLOCKS - 1, j).wait_send()


def solution(mesh):
    n = mesh.shape["tp"]

    def step(x, w_gate, w_up, w_down):
        rows, depth = x.shape
        units = w_gate.shape[1]
        cols = depth // NT
        dma = pltpu.SemaphoreType.DMA
        return pl.pallas_call(
            functools.partial(kernel, n),
            name="mlp",
            out_shape=pltpu.VMEM((rows, depth), BF16),
            in_specs=[pl.BlockSpec(memory_space=pl.ANY)] * 4,
            out_specs=pl.BlockSpec(memory_space=pltpu.VMEM),
            scratch_shapes=[
                pltpu.VMEM((BLOCKS, 2 * rows, depth), BF16),
                pltpu.VMEM((2, 2, depth, FT), BF16),
                pltpu.VMEM((2, units, cols), BF16),
                pltpu.VMEM((2 * rows, units), BF16),
                pltpu.VMEM((2, rows, cols), F32),
                pltpu.VMEM((rows, depth), F32),
                pltpu.VMEM((2, rows, cols), BF16),
                pltpu.VMEM((BLOCKS, rows, depth), BF16),
                pltpu.VMEM((3, rows, depth), BF16),
                dma((2,)), dma((2,)), dma((2,)),
                dma, dma((PIECES + 2,)),
                dma, dma((2,)),
                dma((2,)), dma, dma((2, NT)),
                dma, dma((2, 2)),
            ],
            compiler_params=pltpu.CompilerParams(
                collective_id=0, has_side_effects=True, vmem_limit_bytes=62914560
            ),
        )(x, w_gate, w_up, w_down)

    return jax.shard_map(
        step,
        mesh=mesh,
        in_specs=(P(("dp", "tp"), None), P(None, "tp"), P(None, "tp"), P("tp", None)),
        out_specs=P(("dp", "tp"), None),
        check_vma=False,
    )
```
